32 devices in a mesh: member: 4 (over y, x), lat: 2 (over core), lon: 4 (over z).
Axes of the slice: x: 2, y: 2, z: 4, core: 2. Of those that a mesh axis runs over, the one named last changes fastest.
Arguments:
- ice_flux: float32 [8, 64, 8, 512], P(('member', 'lat'), 'lon'), parts along dimension 0, may hold values from 0.5 to 1.5
- ice_frac: float32 [8, 64, 512], P(('member', 'lat'), 'lon'), parts along dimension 0, may hold values from 0.05 to 1
- ice_mask: int32 [8, 64, 512], P(('member', 'lat'), 'lon'), parts along dimension 0, may hold values 0 or 1
- ice_area: float32 [8, 64, 512], P(('member', 'lat'), 'lon'), parts along dimension 0, may hold values from 0.7 to 44.3
- route: int32 [8, 64], P(('member', 'lat'), 'lon'), parts along dimension 0, may hold values from 0 to 63, as said below
- ocean_area: float32 [512, 512], P(('member', 'lat'), 'lon'), parts along dimension 0, may hold values from 0.7 to 44.3
- ocean_wet: int32 [512, 512], P(('member', 'lat'), 'lon'), parts along dimension 0, may hold values 0 or 1
- exponent: int32 [8], replicated, may hold values from 0 to 3
Outputs:
- ocean_flux: float32 [8, 512, 512], P(None, ('member', 'lat'), 'lon'), parts along dimension 1
- source_total: float32 [32], P('member'), parts along dimension 0
The draws below stay inside these ranges and needn't reach their ends.
There are 4 independent parts, one for each index of `member`. The reference program is written for one: setup_inputs(seed, part) draws one part's arguments, and reference() takes and returns one part's arrays. A program takes and returns all parts, laid end to end along the dimension named above; an argument that names none is the same for every part. Nothing has to cross between parts.
Inputs may be any that keep to these rules, and one draw needn't show every extreme that they name: Within each latitude tile row, route is a permutation of 0 to 63. The 16 entries of one device name, for every longitude tile k that they name (route // 16 == k), exactly 4 blocks of it.
All inputs are finite; a program needn't handle non-finite values. No bound on the sum of `ice_mask` or of `ocean_wet` on one device may be relied on, other than what follows from the above.
Results may differ from the reference program's by a relative error of at most 0.0003.
Values sent between devices are 32-bit elements; how exact they have to be, the bound alone decides.
A program may use at most 64 MiB of HBM per device.

```python
import jax
import jax.numpy as jnp

NF = 8
NBT = 16
BLAT = 4
CLON = 128
CLAT = 64
NLATG = 128
NLONG = 512
N_LAT = 2
N_LON = 4


def shuffled(subkey):
    return jax.random.permutation(subkey, jnp.arange(NBT, dtype=jnp.int32))


def offsets_for(subkey):
    return jax.random.permutation(subkey, jnp.arange(N_LON, dtype=jnp.int32))[:NBT // max(2, NBT // N_LON)]


def make_route(key):
    capacity = max(2, NBT // N_LON)
    offset_count = NBT // capacity
    key_offsets, key_slots, key_positions = jax.random.split(jax.random.fold_in(key, 11), 3)
    offsets = jax.vmap(offsets_for)(jax.random.split(key_offsets, N_LAT))
    sequence = jax.vmap(shuffled)(jax.random.split(key_slots, N_LAT * N_LON)).reshape(N_LAT, N_LON, NBT)
    kind_index = sequence // capacity
    offset_table = jnp.broadcast_to(offsets[:, None, :], (N_LAT, N_LON, offset_count))
    chosen = jnp.take_along_axis(offset_table, kind_index, axis=2)
    source_tile = jnp.arange(N_LON, dtype=jnp.int32)[None, :, None]
    target_tile = (source_tile + chosen) % N_LON
    target_positions = jax.vmap(shuffled)(jax.random.split(key_positions, N_LAT * N_LON)).reshape(-1)
    row_number_index = jnp.arange(N_LAT, dtype=jnp.int32)[:, None, None]
    flat_index = (row_number_index * N_LON + target_tile) * NBT + sequence
    block_row = target_positions[flat_index]
    return (target_tile * NBT + block_row).reshape(N_LAT, N_LON * NBT).astype(jnp.int32)


def area_noise(key, shape):
    return jnp.exp(jax.random.uniform(key, shape, jnp.float32, jnp.log(0.7), jnp.log(1.4)))


def profile(lat_cell, lon_cell):
    return jnp.power(10.0, (lat_cell + 0.5) / NLATG) * jnp.power(10.0, 0.5 * (lon_cell + 0.5) / NLONG)


def draw_route(key, part):
    return make_route(key)


def draw_ice_area(key, part):
    route = make_route(key)
    target_tile = route // NBT
    block_row = route % NBT
    within = jnp.arange(BLAT * CLON, dtype=jnp.int32)
    lat_cell = jnp.arange(N_LAT, dtype=jnp.int32)[:, None, None] * CLAT + block_row[:, :, None] * BLAT + (within // CLON)[None, None, :]
    lon_cell = target_tile[:, :, None] * CLON + (within % CLON)[None, None, :]
    reshaped_grid = profile(lat_cell.astype(jnp.float32), lon_cell.astype(jnp.float32))
    return (reshaped_grid * area_noise(jax.random.fold_in(key, 23), reshaped_grid.shape)).astype(jnp.float32)


def draw_ocean_area(key, part):
    lat_cell = jnp.arange(NLATG, dtype=jnp.int32).astype(jnp.float32)[:, None]
    lon_cell = jnp.arange(NLONG, dtype=jnp.int32).astype(jnp.float32)[None, :]
    reshaped_grid = profile(lat_cell, lon_cell)
    return (reshaped_grid * area_noise(jax.random.fold_in(key, 31), reshaped_grid.shape)).astype(jnp.float32)


def touch_ends(entries, rng, low, top_value):
    longest = entries.shape.index(max(entries.shape))
    spots = []
    for shift in (0, 1):
        where = [jax.random.randint(jax.random.fold_in(rng, axis), (), 0, length) for axis, length in enumerate(entries.shape)]
        where[longest] = (where[longest] + shift) % entries.shape[longest]
        spots.append(tuple(where))
    return entries.at[spots[0]].set(low).at[spots[1]].set(top_value)


def steps_of(stream_key, shape, cuts, smallest, top_value):
    loudness, own = 1.0, jax.random.fold_in(stream_key, 6)
    for axis_at, parts in cuts:
        steps = jnp.exp(jax.random.uniform(jax.random.fold_in(own, axis_at), (parts,), jnp.float32, smallest / len(cuts), top_value / len(cuts)))
        loudness = loudness * jnp.repeat(steps, shape[axis_at] // parts).reshape([-1 if axis == axis_at else 1 for axis in range(len(shape))])
    return loudness


def setup_inputs(seed: int = 0, part: int = 0) -> dict:
    splits = jax.random.split(jax.random.key(seed), 9)
    own_keys = jax.random.split(jax.random.fold_in(splits[8], part), 9)
    ice_flux = jnp.clip(0.5 + 1.0 * jax.random.uniform(own_keys[0], (N_LAT, N_LON * NBT, NF, BLAT * CLON), jnp.float32) ** steps_of(own_keys[0], (N_LAT, N_LON * NBT, NF, BLAT * CLON), ((0, 2), (1, 4)), -0.2, 0.2), 0.5, 1.5)
    ice_frac = jnp.clip(0.05 + 0.95 * jax.random.uniform(own_keys[1], (N_LAT, N_LON * NBT, BLAT * CLON), jnp.float32) ** steps_of(own_keys[1], (N_LAT, N_LON * NBT, BLAT * CLON), ((0, 2), (1, 4)), -0.2, 0.2), 0.05, 1.0)
    ice_mask = touch_ends((jax.random.randint(own_keys[2], (N_LAT, N_LON * NBT, BLAT * CLON), 0, 4) < 3).astype(jnp.int32), jax.random.fold_in(own_keys[2], 1), 0, 1)
    ice_area = draw_ice_area(jax.random.fold_in(jax.random.fold_in(splits[8], part), 71), part)
    route = draw_route(jax.random.fold_in(jax.random.fold_in(splits[8], part), 71), part)
    ocean_area = draw_ocean_area(jax.random.fold_in(jax.random.fold_in(splits[8], part), 71), part)
    ocean_wet = touch_ends((jax.random.randint(own_keys[6], (NLATG, NLONG), 0, 4) < 3).astype(jnp.int32), jax.random.fold_in(own_keys[6], 1), 0, 1)
    exponent = touch_ends(jax.random.randint(splits[7], (NF,), 0, 4), jax.random.fold_in(splits[7], 1), 0, 3).astype(jnp.int32)
    return {"ice_flux": ice_flux, "ice_frac": ice_frac, "ice_mask": ice_mask, "ice_area": ice_area, "route": route, "ocean_area": ocean_area, "ocean_wet": ocean_wet, "exponent": exponent}


quantum = 1024.0
limb_base = 65536


def local_units(values, axes):
    return jnp.sum((values * quantum).astype(jnp.int32), axis=axes)


def split_units(total):
    upper_part = total // limb_base
    return upper_part, total - upper_part * limb_base


def join_units(upper_part, lower_part):
    return (upper_part.astype(jnp.float32) * limb_base + lower_part.astype(jnp.float32)) / quantum


def global_integral(units, axes):
    upper_part, lower_part = split_units(units)
    return join_units(jnp.sum(upper_part, axis=axes), jnp.sum(lower_part, axis=axes))


def reference(ice_flux, ice_frac, ice_mask, ice_area, route, ocean_area, ocean_wet, exponent):
    amount = ice_area * ice_frac * ice_mask.astype(jnp.float32)
    carried = ice_flux * amount[:, :, None, :]
    per_device = carried.reshape(N_LAT, N_LON, NBT, NF, BLAT * CLON)
    source = global_integral(local_units(per_device, (2, 4)), (0, 1))
    row_number_index = jnp.broadcast_to(jnp.arange(N_LAT, dtype=jnp.int32)[:, None], route.shape)
    block_groups = jnp.zeros_like(carried).at[row_number_index, route].set(carried)
    mapped = block_groups.reshape(N_LAT, N_LON, NBT, NF, BLAT, CLON).transpose(3, 0, 2, 4, 1, 5).reshape(NF, NLATG, NLONG)
    wet_cover = ocean_wet.astype(jnp.float32)
    wet_cell_terms = (wet_cover * mapped).reshape(NF, N_LAT, CLAT, N_LON, CLON)
    target = global_integral(local_units(wet_cell_terms, (2, 4)), (1, 2))
    area_terms = (ocean_area * wet_cover).reshape(N_LAT, CLAT, N_LON, CLON)
    wet_area = global_integral(local_units(area_terms, (1, 3)), (0, 1))
    correction = (source - target) / wet_area
    scaling = jnp.left_shift(jnp.ones_like(exponent), exponent).astype(jnp.float32)
    ocean_flux = wet_cover * scaling[:, None, None] * (mapped / ocean_area + correction[:, None, None])
    return ocean_flux, source * scaling
```

```python
import functools

import jax
import jax.numpy as jnp
from jax import lax
from jax.experimental import pallas as pl
from jax.experimental.pallas import tpu as pltpu
from jax.sharding import PartitionSpec as P

MESH = pl.DeviceIdType.MESH
quantum = 1024.0
limb_bits = 16
limb_base = 65536.0
lanes = 128


def carry(upper, lower):
    over = jnp.floor(lower * (1.0 / limb_base))
    return upper + over, lower - over * limb_base


def row_limbs(units):
    upper = jnp.sum((units >> limb_bits).astype(jnp.float32), axis=1, keepdims=True)
    lower = jnp.sum((units & 0xFFFF).astype(jnp.float32), axis=1, keepdims=True)
    return carry(upper, lower)


def join(upper, lower):
    return (upper * limb_base + lower) / quantum


def send_steps(count):
    table = []
    for me in range(count):
        near = sorted((p for p in range(count) if p != me), key=lambda p: (abs(p - me), p))
        table.append(near[-1:] + near[:-1])
    return [[row[step] for row in table] for step in range(count - 1)]


def kernel(
    n_lat, n_lon, cap,
    flux_hbm, frac_hbm, mask_hbm, area_hbm, route_hbm, sea_hbm, wet_hbm, exp_hbm,
    ordered, wetf, coefs, total_ref,
    flux, frac, mask, area, sea, wet, inverse, outgoing, received, routes, exps, sums,
    in_sem, route_send, route_recv, bulk_send, bulk_recv, sum_send, sum_recv,
):
    blocks, fields, cells = flux.shape
    rows, width = sea.shape
    band = cells // width
    bits = blocks.bit_length()
    digit = (1 << bits) - 1
    full = cap * n_lon == blocks
    group = n_lat * n_lon
    my_lat = lax.axis_index("lat")
    me = lax.axis_index("lon")

    def peer(offset):
        return {
            "lat": lax.rem(my_lat + offset // n_lon, n_lat),
            "lon": lax.rem(me + offset % n_lon, n_lon),
        }

    loads = [
        pltpu.make_async_copy(src, dst, in_sem.at[i])
        for i, (src, dst) in enumerate((
            (route_hbm, routes.at[pl.ds(0, 1)]), (area_hbm, area), (frac_hbm, frac),
            (mask_hbm, mask), (flux_hbm, flux), (sea_hbm, sea), (wet_hbm, wet), (exp_hbm, exps),
        ))
    ]
    for load in loads:
        load.start()

    barrier = pltpu.get_barrier_semaphore()
    for offset in range(1, group):
        pl.semaphore_signal(barrier, inc=1, device_id=peer(offset), device_id_type=MESH)

    loads[0].wait()

    def digits_of(slot, low, value):
        packed = jnp.int32(0)
        for s in range(blocks):
            r = routes[slot, s]
            hit = (r >= low) & (r < low + blocks)
            packed = jnp.where(hit, (packed << bits) + (value(s, r - low) + 1), packed)
        return [(packed >> (bits * (cap - 1 - c))) & digit for c in range(cap)]

    pl.semaphore_wait(barrier, group - 1)

    if n_lon ** n_lon < 2 ** 31:
        place = 1
        for i in range(n_lon - 1):
            place = place * (1 + (n_lon - 1) * ((me + n_lon - 1 - i) // n_lon))
        steps = [
            sum(t * n_lon ** i for i, t in enumerate(row)) // place % n_lon
            for row in send_steps(n_lon)
        ]
    else:
        steps = [lax.rem(me + d, n_lon) for d in range(1, n_lon)]
    away = [lax.rem(target - me + n_lon, n_lon) for target in steps]

    def lon_copy(src, dst, send, recv, d, target):
        return pltpu.make_async_remote_copy(
            src_ref=src, dst_ref=dst, send_sem=send.at[d - 1], recv_sem=recv.at[d - 1],
            device_id={"lat": my_lat, "lon": target}, device_id_type=MESH,
        )

    route_copies = [
        lon_copy(routes.at[pl.ds(0, 1)], routes.at[pl.ds(d, 1)], route_send, route_recv, d, t)
        for d, t in zip(away, steps)
    ]
    for copy in route_copies:
        copy.start()

    chosen = [
        [jnp.maximum(v - 1, 0) for v in digits_of(0, target * blocks, lambda s, row: s)]
        for target in steps + [me]
    ]
    for load in loads[1:5]:
        load.wait()

    bulk = []
    for step, picks in enumerate(chosen):
        last = step == n_lon - 1
        for c, s in enumerate(picks):
            here = pl.ds(s, 1)
            amount = area[here, :] * frac[here, :] * mask[here, :].astype(jnp.float32)
            block = flux[s] * amount
            if last:
                received[c] = block
            else:
                outgoing[step * cap + c] = block
        if not last:
            d = away[step]
            bulk.append(lon_copy(
                outgoing.at[pl.ds(step * cap, cap)], received.at[pl.ds(d * cap, cap)],
                bulk_send, bulk_recv, d, steps[step],
            ))
            bulk[-1].start()

    def arrival(d):
        here = received.at[pl.ds(d * cap, cap)]
        line = routes.at[pl.ds(d, 1)]
        source = lax.rem(me - d + n_lon, n_lon)
        return (
            lon_copy(line, line, route_send, route_recv, d, source),
            lon_copy(here, here, bulk_send, bulk_recv, d, source),
        )

    source_units = jnp.zeros((fields, width), jnp.int32)
    for s in range(blocks):
        here = pl.ds(s, 1)
        amount = area[here, :] * frac[here, :] * mask[here, :].astype(jnp.float32)
        units = (flux[s] * amount * quantum).astype(jnp.int32)
        for r in range(band):
            source_units += units[:, r * width : (r + 1) * width]

    for load in loads[5:]:
        load.wait()
    wetf[...] = wet[...].astype(jnp.float32)
    inverse[...] = wetf[...] / sea[...]
    area_units = jnp.zeros((8, width), jnp.int32)
    for i in range(rows // 8):
        part = pl.ds(i * 8, 8)
        area_units += (sea[part, :] * wetf[part, :] * quantum).astype(jnp.int32)

    sub = lax.broadcasted_iota(jnp.int32, (8, lanes), 0)
    lane = lax.broadcasted_iota(jnp.int32, (8, lanes), 1)

    def placed(values, first):
        return sum(
            jnp.where(lane == sub + (first + i) * 8, v, 0.0) for i, v in enumerate(values)
        )

    early = placed(row_limbs(source_units) + row_limbs(area_units), 0)
    power = jnp.zeros((8, lanes), jnp.int32)
    power_row = jnp.zeros((1, lanes), jnp.int32)
    for f in range(fields):
        power = jnp.where(sub == f, exps[f], power)
        power_row = jnp.where(lane[:1] == f, exps[f], power_row)
    scaling = jnp.left_shift(jnp.ones_like(power), power).astype(jnp.float32)
    scaling_row = jnp.left_shift(jnp.ones_like(power_row), power_row).astype(jnp.float32)

    low = me * blocks
    slot_of = [jnp.int32(0)] * blocks
    target_units = jnp.zeros((fields, width), jnp.int32)
    near_first = sorted(range(n_lon), key=lambda d: min(d, n_lon - d))
    for d in near_first:
        if d:
            route_arrival, bulk_arrival = arrival(d)
            route_arrival.wait_recv()
        digits = digits_of(d, low, lambda s, row: row)
        for c in range(cap):
            for n in range(blocks):
                slot_of[n] = jnp.where(digits[c] == n + 1, d * cap + c, slot_of[n])
        if d:
            bulk_arrival.wait_recv()
        for c in range(cap):
            row = jnp.maximum(digits[c] - 1, 0)
            for r in range(band):
                cover = wetf[pl.ds(row * band + r, 1), :]
                value = received[d * cap + c, :, r * width : (r + 1) * width]
                units = (cover * value * quantum).astype(jnp.int32)
                if not full:
                    units = units * jnp.minimum(digits[c], 1)
                target_units += units

    mine = jnp.sum(early + placed(row_limbs(target_units), 4), axis=0, keepdims=True)
    sums[pl.ds(0, 1), :] = mine
    sum_copies = []
    for offset in range(1, group):
        copy = pltpu.make_async_remote_copy(
            src_ref=sums.at[pl.ds(0, 1)], dst_ref=sums.at[pl.ds(offset, 1)],
            send_sem=sum_send.at[offset - 1], recv_sem=sum_recv.at[offset - 1],
            device_id=peer(offset), device_id_type=MESH,
        )
        copy.start()
        sum_copies.append(copy)
    for n in range(blocks):
        slot = slot_of[n]
        for r in range(band):
            line = n * band + r
            value = received[slot, :, r * width : (r + 1) * width]
            ordered[pl.ds(line, fields, stride=rows), :] = value * inverse[line : line + 1, :]

    for copy in sum_copies:
        copy.wait_recv()

    whole = jnp.sum(sums[...], axis=0, keepdims=True)

    def taken(i):
        return jnp.sum(jnp.where(lane == sub + i * 8, whole, 0.0), axis=1, keepdims=True)

    source = join(taken(0), taken(1))
    wet_upper, wet_lower = carry(taken(2), taken(3))
    wet_area = join(
        jnp.sum(wet_upper, axis=0, keepdims=True), jnp.sum(wet_lower, axis=0, keepdims=True)
    )
    target = join(taken(4), taken(5))
    coefs[0] = scaling
    coefs[1] = scaling * ((source - target) / wet_area)

    aligned = pltpu.roll(whole, lanes - 8, 1)
    total_ref[...] = join(whole, aligned) * scaling_row

    for copy in sum_copies + route_copies + bulk:
        copy.wait_send()


def finish(ordered, wetf, coefs, total_row, out_hbm, total_hbm, out, total, sems):
    fields = total.shape[0]
    rows = wetf.shape[0]
    total[...] = total_row[0, :fields]
    copies = [pltpu.make_async_copy(total, total_hbm, sems.at[fields])]
    copies[0].start()
    for f in range(fields):
        here = pl.ds(f * rows, rows)
        out[here, :] = ordered[here, :] * coefs[0, f : f + 1, :] + wetf[...] * coefs[1, f : f + 1, :]
        copies.append(pltpu.make_async_copy(out.at[here], out_hbm.at[here], sems.at[f]))
        copies[-1].start()
    for copy in copies:
        copy.wait()


def solution(mesh):
    n_lat, n_lon = mesh.shape["lat"], mesh.shape["lon"]

    def body(ice_flux, ice_frac, ice_mask, ice_area, route, ocean_area, ocean_wet, exponent):
        blocks, fields, cells = ice_flux.shape[1:]
        rows, width = ocean_area.shape
        cap = max(2, blocks // n_lon)
        group = n_lat * n_lon
        anywhere = pl.BlockSpec(memory_space=pl.ANY)
        vmem = pl.BlockSpec(memory_space=pltpu.VMEM)
        dma = pltpu.SemaphoreType.DMA
        near = pl.pallas_call(
            functools.partial(kernel, n_lat, n_lon, cap),
            out_shape=(
                pltpu.VMEM((fields * rows, width), jnp.float32),
                pltpu.VMEM((rows, width), jnp.float32),
                pltpu.VMEM((2, fields, lanes), jnp.float32),
                pltpu.VMEM((1, lanes), jnp.float32),
            ),
            in_specs=[anywhere] * 8,
            out_specs=(vmem,) * 4,
            scratch_shapes=[
                pltpu.VMEM((blocks, fields, cells), jnp.float32),
                pltpu.VMEM((blocks, cells), jnp.float32),
                pltpu.VMEM((blocks, cells), jnp.int32),
                pltpu.VMEM((blocks, cells), jnp.float32),
                pltpu.VMEM((rows, width), jnp.float32),
                pltpu.VMEM((rows, width), jnp.int32),
                pltpu.VMEM((rows, width), jnp.float32),
                pltpu.VMEM(((n_lon - 1) * cap, fields, cells), jnp.float32),
                pltpu.VMEM((n_lon * cap, fields, cells), jnp.float32),
                pltpu.SMEM((n_lon, blocks), jnp.int32),
                pltpu.SMEM((fields,), jnp.int32),
                pltpu.VMEM((group, lanes), jnp.float32),
                dma((8,)),
                dma((n_lon - 1,)), dma((n_lon - 1,)),
                dma((n_lon - 1,)), dma((n_lon - 1,)),
                dma((group - 1,)), dma((group - 1,)),
            ],
            compiler_params=pltpu.CompilerParams(collective_id=0, has_side_effects=True),
        )(
            ice_flux[0], ice_frac[0], ice_mask[0], ice_area[0],
            route, ocean_area, ocean_wet, exponent,
        )
        flux_out, total = pl.pallas_call(
            finish,
            out_shape=(
                jax.ShapeDtypeStruct((fields * rows, width), jnp.float32),
                jax.ShapeDtypeStruct((fields,), jnp.float32),
            ),
            in_specs=[vmem] * 4,
            out_specs=(anywhere, anywhere),
            scratch_shapes=[
                pltpu.VMEM((fields * rows, width), jnp.float32),
                pltpu.VMEM((fields,), jnp.float32),
                dma((fields + 1,)),
            ],
        )(*(pltpu.with_memory_space_constraint(x, pltpu.VMEM) for x in near))
        return flux_out.reshape(fields, rows, width), total

    placed = (
        P(("member", "lat"), "lon", None, None),
        P(("member", "lat"), "lon", None),
        P(("member", "lat"), "lon", None),
        P(("member", "lat"), "lon", None),
        P(("member", "lat"), "lon"),
        P(("member", "lat"), "lon"),
        P(("member", "lat"), "lon"),
        P(),
    )
    return jax.shard_map(
        body,
        mesh=mesh,
        in_specs=placed,
        out_specs=(P(None, ("member", "lat"), "lon"), P("member")),
        check_vma=False,
    )
```

```python
import functools

import jax
import jax.numpy as jnp
from jax import lax
from jax.experimental import pallas as pl
from jax.experimental.pallas import tpu as pltpu
from jax.sharding import PartitionSpec as P

MESH = pl.DeviceIdType.MESH
quantum = 1024.0
limb_bits = 16
limb_base = 65536.0
lanes = 128


def carry(upper, lower):
    over = jnp.floor(lower * (1.0 / limb_base))
    return upper + over, lower - over * limb_base


def row_limbs(units):
    upper = jnp.sum((units >> limb_bits).astype(jnp.float32), axis=1, keepdims=True)
    lower = jnp.sum((units & 0xFFFF).astype(jnp.float32), axis=1, keepdims=True)
    return carry(upper, lower)


def join(upper, lower):
    return (upper * limb_base + lower) / quantum


PLANS = {
    4: (
        (4, 6, 7, 5, 2, 3),
        (4, 6, 7, 0, 1, 5),
        (2, 3, 0, 1, 6, 7),
        (2, 3, 0, 1, 4, 5),
        (2, 4, 6, -8, 5, 3),
        (4, 5, 6, -8, 0, 1),
        (2, 0, 1, 3, 6, 7),
        (2, 0, 1, 3, 4, 5),
    ),
}
EARLY = 3
PARTS = 2


def send_plan(count):
    rows = PLANS.get(count)
    if rows is None:
        rows = [
            [
                target * PARTS + half
                for target in sorted((p for p in range(count) if p != me), key=lambda p: -abs(p - me))
                for half in range(PARTS)
            ]
            for _ in range(2)
            for me in range(count)
        ]
    codes = [[(code if code >= 0 else ~code, code < 0) for code in row] for row in rows]
    return [[(code // PARTS, code % PARTS, hold) for code, hold in row] for row in codes]


def kernel(
    n_lat, n_lon, cap,
    flux_hbm, frac_hbm, mask_hbm, area_hbm, route_hbm, sea_hbm, wet_hbm, exp_hbm,
    ordered, wetf, coefs, total_ref,
    flux, frac, mask, area, sea, wet, inverse, outgoing, received, routes, exps, tally,
    in_sem, route_send, route_recv, bulk_send, bulk_recv, tally_send, early_recv, late_recv, top_in, go,
):
    blocks, fields, cells = flux.shape
    rows, width = sea.shape
    band = cells // width
    bits = blocks.bit_length()
    digit = (1 << bits) - 1
    full = cap * n_lon == blocks
    group = n_lat * n_lon
    piece = cap // PARTS
    my_lat = lax.axis_index("lat")
    me = lax.axis_index("lon")

    def peer(offset):
        return {
            "lat": lax.rem(my_lat + offset // n_lon, n_lat),
            "lon": lax.rem(me + offset % n_lon, n_lon),
        }

    loads = [
        pltpu.make_async_copy(src, dst, in_sem.at[i])
        for i, (src, dst) in enumerate((
            (route_hbm, routes.at[pl.ds(0, 1)]), (area_hbm, area), (frac_hbm, frac),
            (mask_hbm, mask), (flux_hbm, flux), (sea_hbm, sea), (wet_hbm, wet), (exp_hbm, exps),
        ))
    ]
    for load in loads:
        load.start()

    top = n_lon - 1
    barrier = pltpu.get_barrier_semaphore()
    for offset in range(1, n_lat):
        pl.semaphore_signal(barrier, inc=1, device_id=peer(offset * n_lon), device_id_type=MESH)

    @pl.when(me < top)
    def _():
        for offset in range(1, n_lon):
            pl.semaphore_signal(barrier, inc=1, device_id=peer(offset), device_id_type=MESH)

    @pl.when(me == top)
    def _():
        pl.semaphore_wait(barrier, n_lat + n_lon - 2)
        for z in range(top):
            pl.semaphore_signal(
                top_in, inc=1, device_id={"lat": my_lat, "lon": z}, device_id_type=MESH
            )

    loads[0].wait()

    def digits_of(slot, low, value):
        packed = jnp.int32(0)
        for s in range(blocks):
            r = routes[slot, s]
            hit = (r >= low) & (r < low + blocks)
            packed = jnp.where(hit, (packed << bits) + (value(s, r - low) + 1), packed)
        return [(packed >> (bits * (cap - 1 - c))) & digit for c in range(cap)]

    kind = lax.rem(my_lat, 2) if n_lat > 1 else jnp.int32(0)
    place = kind * n_lon + me

    def mine_of(values):
        out = jnp.int32(values[0])
        for z, v in enumerate(values):
            if v != values[0]:
                out = jnp.where(place == z, jnp.int32(v), out)
        return out

    plans = send_plan(n_lon)
    entries = len(plans[0])
    targets = [mine_of([plan[k][0] for plan in plans]) for k in range(entries)]
    halves = [mine_of([plan[k][1] for plan in plans]) for k in range(entries)]
    holds = [[plan[k][2] for plan in plans] for k in range(entries)]
    firsts = [
        [plan[k][0] not in [e[0] for e in plan[:k]] for plan in plans] for k in range(entries)
    ]
    order = [list(dict.fromkeys(e[0] for e in plan)) for plan in plans]
    steps = [mine_of([row[i] for row in order]) for i in range(n_lon - 1)]

    def lon_copy(src, dst, send, recv, d, target):
        return pltpu.make_async_remote_copy(
            src_ref=src, dst_ref=dst, send_sem=send, recv_sem=recv,
            device_id={"lat": my_lat, "lon": target}, device_id_type=MESH,
        )

    def route_copy(target):
        d = lax.rem(target - me + n_lon, n_lon)
        return lon_copy(routes.at[pl.ds(0, 1)], routes.at[pl.ds(d, 1)], route_send, route_recv, d, target)

    def bulk_copy(k):
        d = lax.rem(targets[k] - me + n_lon, n_lon)
        return pltpu.make_async_remote_copy(
            src_ref=outgoing.at[pl.ds(targets[k] * cap + halves[k] * piece, piece)],
            dst_ref=received.at[pl.ds(d * cap + halves[k] * piece, piece)],
            send_sem=bulk_send.at[int(k >= EARLY)], recv_sem=bulk_recv.at[d - 1],
            device_id={"lat": my_lat, "lon": targets[k]}, device_id_type=MESH,
        )

    def all_of(ref, send, recv):
        return pltpu.make_async_remote_copy(
            src_ref=ref, dst_ref=ref, send_sem=send, recv_sem=recv,
            device_id=peer(1), device_id_type=MESH,
        )

    chosen = [
        [jnp.maximum(v - 1, 0) for v in digits_of(0, target * blocks, lambda s, row: s)]
        for target in steps + [me]
    ]
    for load in loads[1:5]:
        load.wait()

    def fill(target, picks):
        for c, s in enumerate(picks):
            here = pl.ds(s, 1)
            amount = area[here, :] * frac[here, :] * mask[here, :].astype(jnp.float32)
            outgoing[target * cap + c] = flux[s] * amount

    bulk = [bulk_copy(k) for k in range(entries)]
    first_part = all_of(outgoing.at[pl.ds(0, EARLY * piece)], bulk_send.at[0], bulk_recv.at[0])
    rest_part = all_of(
        outgoing.at[pl.ds(0, (entries - EARLY) * piece)], bulk_send.at[1], bulk_recv.at[0]
    )

    def send(k):
        if any(holds[k]):
            @pl.when(mine_of(holds[k]) == 1)
            def _():
                pl.semaphore_wait(go, 1)

        waits = [
            first and plan[k][0] == top
            for z, (first, plan) in enumerate(zip(firsts[k], plans))
        ]
        if any(waits):
            @pl.when(mine_of(waits) == 1)
            def _():
                pl.semaphore_wait(top_in, 1)

        if all(firsts[k]):
            route_copy(targets[k]).start()
        elif any(firsts[k]):
            @pl.when(mine_of(firsts[k]) == 1)
            def _():
                route_copy(targets[k]).start()

        bulk[k].start()

    fill(steps[0], chosen[0])
    @pl.when(me < top)
    def _():
        pl.semaphore_wait(barrier, n_lat + n_lon - 3)

    @pl.when(kind == 0)
    def _():
        send(0)

    for target, picks in zip(steps[1:], chosen[1:-1]):
        fill(target, picks)

    @pl.when(kind == 0)
    def _():
        for k in range(1, entries):
            send(k)

    @pl.when(kind == 1)
    def _():
        for k in range(EARLY):
            send(k)

    for c, s in enumerate(chosen[-1]):
        here = pl.ds(s, 1)
        amount = area[here, :] * frac[here, :] * mask[here, :].astype(jnp.float32)
        received[c] = flux[s] * amount

    source_units = jnp.zeros((fields, width), jnp.int32)
    for s in range(blocks):
        here = pl.ds(s, 1)
        amount = area[here, :] * frac[here, :] * mask[here, :].astype(jnp.float32)
        units = (flux[s] * amount * quantum).astype(jnp.int32)
        for r in range(band):
            source_units += units[:, r * width : (r + 1) * width]

    for load in loads[5:]:
        load.wait()
    wetf[...] = wet[...].astype(jnp.float32)
    inverse[...] = wetf[...] / sea[...]
    area_units = jnp.zeros((8, width), jnp.int32)
    for i in range(rows // 8):
        part = pl.ds(i * 8, 8)
        area_units += (sea[part, :] * wetf[part, :] * quantum).astype(jnp.int32)

    held = [any(e[2] for e in plan) for plan in plans[n_lon:]]
    frees = mine_of(held + [False] * n_lon)
    if n_lat > 1 and any(held):
        @pl.when(frees == 1)
        def _():
            first_part.wait_send()
            pl.semaphore_signal(
                go, inc=1, device_id={"lat": my_lat + 1, "lon": me}, device_id_type=MESH
            )

    @pl.when(kind == 1)
    def _():
        for k in range(EARLY, entries):
            send(k)

    sub = lax.broadcasted_iota(jnp.int32, (8, lanes), 0)
    lane = lax.broadcasted_iota(jnp.int32, (8, lanes), 1)

    def placed(values, first):
        return sum(
            jnp.where(lane == sub + (first + i) * 8, v, 0.0) for i, v in enumerate(values)
        )

    firsts_row = placed(row_limbs(source_units) + row_limbs(area_units), 0)
    tally[pl.ds(0, 1), :] = jnp.sum(firsts_row, axis=0, keepdims=True)
    power = jnp.zeros((8, lanes), jnp.int32)
    power_row = jnp.zeros((1, lanes), jnp.int32)
    for f in range(fields):
        power = jnp.where(sub == f, exps[f], power)
        power_row = jnp.where(lane[:1] == f, exps[f], power_row)
    scaling = jnp.left_shift(jnp.ones_like(power), power).astype(jnp.float32)
    scaling_row = jnp.left_shift(jnp.ones_like(power_row), power_row).astype(jnp.float32)

    low = me * blocks
    slot_of = [jnp.int32(0)] * blocks
    near_first = sorted(range(n_lon), key=lambda d: min(d, n_lon - d))
    found = {}
    for d in near_first:
        if len(found) == 1:
            all_of(routes.at[pl.ds(1, n_lon - 1)], route_send, route_recv).wait_recv()
        found[d] = digits_of(d, low, lambda s, row: row)
        for c in range(cap):
            for n in range(blocks):
                slot_of[n] = jnp.where(found[d][c] == n + 1, d * cap + c, slot_of[n])

    def spread(base, recv):
        for offset in range(1, group):
            pltpu.make_async_remote_copy(
                src_ref=tally.at[pl.ds(base, 1)], dst_ref=tally.at[pl.ds(base + offset, 1)],
                send_sem=tally_send, recv_sem=recv,
                device_id=peer(offset), device_id_type=MESH,
            ).start()
        return all_of(tally.at[pl.ds(base + 1, group - 1)], tally_send, recv)

    early_rows = spread(0, early_recv)

    target_units = jnp.zeros((fields, width), jnp.int32)
    for d in near_first:
        if d:
            all_of(received.at[pl.ds(d * cap, cap)], bulk_send.at[0], bulk_recv.at[d - 1]).wait_recv()
        for c in range(cap):
            row = jnp.maximum(found[d][c] - 1, 0)
            for r in range(band):
                cover = wetf[pl.ds(row * band + r, 1), :]
                value = received[d * cap + c, :, r * width : (r + 1) * width]
                units = (cover * value * quantum).astype(jnp.int32)
                if not full:
                    units = units * jnp.minimum(found[d][c], 1)
                target_units += units

    tally[pl.ds(group, 1), :] = jnp.sum(placed(row_limbs(target_units), 0), axis=0, keepdims=True)
    late_rows = spread(group, late_recv)
    for n in range(blocks):
        slot = slot_of[n]
        for r in range(band):
            line = n * band + r
            value = received[slot, :, r * width : (r + 1) * width]
            ordered[pl.ds(line, fields, stride=rows), :] = value * inverse[line : line + 1, :]

    def taken(whole, i):
        return jnp.sum(jnp.where(lane == sub + i * 8, whole, 0.0), axis=1, keepdims=True)

    early_rows.wait_recv()
    whole = jnp.sum(tally[pl.ds(0, group), :], axis=0, keepdims=True)
    source = join(taken(whole, 0), taken(whole, 1))
    wet_upper, wet_lower = carry(taken(whole, 2), taken(whole, 3))
    wet_area = join(
        jnp.sum(wet_upper, axis=0, keepdims=True), jnp.sum(wet_lower, axis=0, keepdims=True)
    )
    coefs[0] = scaling
    share = scaling / wet_area
    total_ref[...] = join(whole, pltpu.roll(whole, lanes - 8, 1)) * scaling_row

    late_rows.wait_recv()
    whole = jnp.sum(tally[pl.ds(group, group), :], axis=0, keepdims=True)
    target = join(taken(whole, 0), taken(whole, 1))
    coefs[1] = (source - target) * share

    all_of(tally.at[pl.ds(0, 2 * (group - 1))], tally_send, late_recv).wait_send()
    all_of(routes.at[pl.ds(1, n_lon - 1)], route_send, route_recv).wait_send()

    @pl.when(frees == 0)
    def _():
        first_part.wait_send()

    rest_part.wait_send()


def finish(ordered, wetf, coefs, total_row, out_hbm, total_hbm, out, total, sems):
    fields = total.shape[0]
    rows = wetf.shape[0]
    total[...] = total_row[0, :fields]
    row = pltpu.make_async_copy(total, total_hbm, sems.at[0])
    row.start()
    for f in range(fields):
        here = pl.ds(f * rows, rows)
        out[here, :] = ordered[here, :] * coefs[0, f : f + 1, :] + wetf[...] * coefs[1, f : f + 1, :]
        pltpu.make_async_copy(out.at[here], out_hbm.at[here], sems.at[1]).start()
    row.wait()
    pltpu.make_async_copy(out, out_hbm, sems.at[1]).wait()


def solution(mesh):
    n_lat, n_lon = mesh.shape["lat"], mesh.shape["lon"]

    def body(ice_flux, ice_frac, ice_mask, ice_area, route, ocean_area, ocean_wet, exponent):
        blocks, fields, cells = ice_flux.shape[1:]
        rows, width = ocean_area.shape
        cap = max(2, blocks // n_lon)
        group = n_lat * n_lon
        anywhere = pl.BlockSpec(memory_space=pl.ANY)
        vmem = pl.BlockSpec(memory_space=pltpu.VMEM)
        dma = pltpu.SemaphoreType.DMA
        near = pl.pallas_call(
            functools.partial(kernel, n_lat, n_lon, cap),
            out_shape=(
                pltpu.VMEM((fields * rows, width), jnp.float32),
                pltpu.VMEM((rows, width), jnp.float32),
                pltpu.VMEM((2, fields, lanes), jnp.float32),
                pltpu.VMEM((1, lanes), jnp.float32),
            ),
            in_specs=[anywhere] * 8,
            out_specs=(vmem,) * 4,
            scratch_shapes=[
                pltpu.VMEM((blocks, fields, cells), jnp.float32),
                pltpu.VMEM((blocks, cells), jnp.float32),
                pltpu.VMEM((blocks, cells), jnp.int32),
                pltpu.VMEM((blocks, cells), jnp.float32),
                pltpu.VMEM((rows, width), jnp.float32),
                pltpu.VMEM((rows, width), jnp.int32),
                pltpu.VMEM((rows, width), jnp.float32),
                pltpu.VMEM((n_lon * cap, fields, cells), jnp.float32),
                pltpu.VMEM((n_lon * cap, fields, cells), jnp.float32),
                pltpu.SMEM((n_lon, blocks), jnp.int32),
                pltpu.SMEM((fields,), jnp.int32),
                pltpu.VMEM((2 * group, lanes), jnp.float32),
                dma((8,)),
                dma, dma, dma((2,)), dma((n_lon - 1,)), dma, dma, dma,
                pltpu.SemaphoreType.REGULAR, pltpu.SemaphoreType.REGULAR,
            ],
            compiler_params=pltpu.CompilerParams(collective_id=0, has_side_effects=True),
        )(
            ice_flux[0], ice_frac[0], ice_mask[0], ice_area[0],
            route, ocean_area, ocean_wet, exponent,
        )
        flux_out, total = pl.pallas_call(
            finish,
            out_shape=(
                jax.ShapeDtypeStruct((fields * rows, width), jnp.float32),
                jax.ShapeDtypeStruct((fields,), jnp.float32),
            ),
            in_specs=[vmem] * 4,
            out_specs=(anywhere, anywhere),
            scratch_shapes=[
                pltpu.VMEM((fields * rows, width), jnp.float32),
                pltpu.VMEM((fields,), jnp.float32),
                dma((2,)),
            ],
        )(*(pltpu.with_memory_space_constraint(x, pltpu.VMEM) for x in near))
        return flux_out.reshape(fields, rows, width), total

    placed = (
        P(("member", "lat"), "lon", None, None),
        P(("member", "lat"), "lon", None),
        P(("member", "lat"), "lon", None),
        P(("member", "lat"), "lon", None),
        P(("member", "lat"), "lon"),
        P(("member", "lat"), "lon"),
        P(("member", "lat"), "lon"),
        P(),
    )
    return jax.shard_map(
        body,
        mesh=mesh,
        in_specs=placed,
        out_specs=(P(None, ("member", "lat"), "lon"), P("member")),
        check_vma=False,
    )
```

```python
import functools

import jax
import jax.numpy as jnp
from jax import lax
from jax.experimental import pallas as pl
from jax.experimental.pallas import tpu as pltpu
from jax.sharding import PartitionSpec as P

MESH = pl.DeviceIdType.MESH
quantum = 1024.0
limb_bits = 16
limb_base = 65536.0
lanes = 128


def carry(upper, lower):
    over = jnp.floor(lower * (1.0 / limb_base))
    return upper + over, lower - over * limb_base


def row_limbs(units):
    upper = jnp.sum((units >> limb_bits).astype(jnp.float32), axis=1, keepdims=True)
    lower = jnp.sum((units & 0xFFFF).astype(jnp.float32), axis=1, keepdims=True)
    return carry(upper, lower)


def join(upper, lower):
    return (upper * limb_base + lower) / quantum


PLANS = {
    4: (
        (4, 6, 7, 5, 2, 3),
        (4, 6, 7, 0, 1, 5),
        (2, 3, 0, 1, 6, 7),
        (2, 3, 0, 1, 4, 5),
        (2, 4, 6, -8, 5, 3),
        (4, 5, 6, -8, 0, 1),
        (2, 0, 1, 3, 6, 7),
        (2, 0, 1, 3, 4, 5),
    ),
}
EARLY = 3
PARTS = 2


def send_plan(count):
    rows = PLANS.get(count)
    if rows is None:
        rows = [
            [
                target * PARTS + half
                for target in sorted((p for p in range(count) if p != me), key=lambda p: -abs(p - me))
                for half in range(PARTS)
            ]
            for _ in range(2)
            for me in range(count)
        ]
    codes = [[(code if code >= 0 else ~code, code < 0) for code in row] for row in rows]
    return [[(code // PARTS, code % PARTS, hold) for code, hold in row] for row in codes]


def kernel(
    n_lat, n_lon, cap,
    flux_hbm, frac_hbm, mask_hbm, area_hbm, route_hbm, sea_hbm, wet_hbm, exp_hbm,
    ordered, wetf, coefs, total_ref,
    flux, frac, mask, area, sea, wet, inverse, outgoing, received, routes, exps, tally,
    in_sem, route_recv, bulk_recv, early_recv, late_recv, top_in, go,
):
    blocks, fields, cells = flux.shape
    rows, width = sea.shape
    band = cells // width
    bits = blocks.bit_length()
    route_send, tally_send, bulk_send = in_sem.at[1], in_sem.at[2], [in_sem.at[3], in_sem.at[4]]
    digit = (1 << bits) - 1
    full = cap * n_lon == blocks
    group = n_lat * n_lon
    piece = cap // PARTS
    my_lat = lax.axis_index("lat")
    me = lax.axis_index("lon")

    def peer(offset):
        return {
            "lat": lax.rem(my_lat + offset // n_lon, n_lat),
            "lon": lax.rem(me + offset % n_lon, n_lon),
        }

    loads = [
        pltpu.make_async_copy(src, dst, in_sem.at[i])
        for i, (src, dst) in enumerate((
            (route_hbm, routes.at[pl.ds(0, 1)]), (area_hbm, area), (frac_hbm, frac),
            (mask_hbm, mask), (flux_hbm, flux), (sea_hbm, sea), (wet_hbm, wet), (exp_hbm, exps),
        ))
    ]
    for load in loads:
        load.start()

    top = n_lon - 1
    barrier = pltpu.get_barrier_semaphore()
    for offset in range(1, n_lat):
        pl.semaphore_signal(barrier, inc=1, device_id=peer(offset * n_lon), device_id_type=MESH)

    @pl.when(me < top)
    def _():
        for offset in range(1, n_lon):
            pl.semaphore_signal(barrier, inc=1, device_id=peer(offset), device_id_type=MESH)

    @pl.when(me == top)
    def _():
        pl.semaphore_wait(barrier, n_lat + n_lon - 2)
        for z in range(top):
            pl.semaphore_signal(
                top_in, inc=1, device_id={"lat": my_lat, "lon": z}, device_id_type=MESH
            )

    loads[0].wait()

    def digits_of(slot, low, value):
        packed = jnp.int32(0)
        for s in range(blocks):
            r = routes[slot, s]
            hit = (r >= low) & (r < low + blocks)
            packed = jnp.where(hit, (packed << bits) + (value(s, r - low) + 1), packed)
        return [(packed >> (bits * (cap - 1 - c))) & digit for c in range(cap)]

    kind = lax.rem(my_lat, 2) if n_lat > 1 else jnp.int32(0)
    place = kind * n_lon + me

    def mine_of(values):
        out = jnp.int32(values[0])
        for z, v in enumerate(values):
            if v != values[0]:
                out = jnp.where(place == z, jnp.int32(v), out)
        return out

    plans = send_plan(n_lon)
    entries = len(plans[0])
    targets = [mine_of([plan[k][0] for plan in plans]) for k in range(entries)]
    halves = [mine_of([plan[k][1] for plan in plans]) for k in range(entries)]
    holds = [[plan[k][2] for plan in plans] for k in range(entries)]
    firsts = [
        [plan[k][0] not in [e[0] for e in plan[:k]] for plan in plans] for k in range(entries)
    ]
    order = [list(dict.fromkeys(e[0] for e in plan)) for plan in plans]
    steps = [mine_of([row[i] for row in order]) for i in range(n_lon - 1)]

    def lon_copy(src, dst, send, recv, d, target):
        return pltpu.make_async_remote_copy(
            src_ref=src, dst_ref=dst, send_sem=send, recv_sem=recv,
            device_id={"lat": my_lat, "lon": target}, device_id_type=MESH,
        )

    def route_copy(target):
        d = lax.rem(target - me + n_lon, n_lon)
        return lon_copy(routes.at[pl.ds(0, 1)], routes.at[pl.ds(d, 1)], route_send, route_recv, d, target)

    def bulk_copy(k):
        d = lax.rem(targets[k] - me + n_lon, n_lon)
        return pltpu.make_async_remote_copy(
            src_ref=outgoing.at[pl.ds(targets[k] * cap + halves[k] * piece, piece)],
            dst_ref=received.at[pl.ds(d * cap + halves[k] * piece, piece)],
            send_sem=bulk_send[int(k >= EARLY)], recv_sem=bulk_recv.at[d - 1],
            device_id={"lat": my_lat, "lon": targets[k]}, device_id_type=MESH,
        )

    def all_of(ref, send, recv):
        return pltpu.make_async_remote_copy(
            src_ref=ref, dst_ref=ref, send_sem=send, recv_sem=recv,
            device_id=peer(1), device_id_type=MESH,
        )

    chosen = [
        [jnp.maximum(v - 1, 0) for v in digits_of(0, target * blocks, lambda s, row: s)]
        for target in steps + [me]
    ]
    for load in loads[1:5]:
        load.wait()

    def fill(target, picks):
        for c, s in enumerate(picks):
            here = pl.ds(s, 1)
            amount = area[here, :] * frac[here, :] * mask[here, :].astype(jnp.float32)
            outgoing[target * cap + c] = flux[s] * amount

    bulk = [bulk_copy(k) for k in range(entries)]
    first_part = all_of(outgoing.at[pl.ds(0, EARLY * piece)], bulk_send[0], bulk_recv.at[0])
    rest_part = all_of(
        outgoing.at[pl.ds(0, (entries - EARLY) * piece)], bulk_send[1], bulk_recv.at[0]
    )

    def send(k):
        if any(holds[k]):
            @pl.when(mine_of(holds[k]) == 1)
            def _():
                pl.semaphore_wait(go, 1)

        waits = [
            first and plan[k][0] == top
            for z, (first, plan) in enumerate(zip(firsts[k], plans))
        ]
        if any(waits):
            @pl.when(mine_of(waits) == 1)
            def _():
                pl.semaphore_wait(top_in, 1)

        if all(firsts[k]):
            route_copy(targets[k]).start()
        elif any(firsts[k]):
            @pl.when(mine_of(firsts[k]) == 1)
            def _():
                route_copy(targets[k]).start()

        bulk[k].start()

    fill(steps[0], chosen[0])
    @pl.when(me < top)
    def _():
        pl.semaphore_wait(barrier, n_lat + n_lon - 3)

    @pl.when(kind == 0)
    def _():
        send(0)

    for target, picks in zip(steps[1:], chosen[1:-1]):
        fill(target, picks)

    @pl.when(kind == 0)
    def _():
        for k in range(1, entries):
            send(k)

    @pl.when(kind == 1)
    def _():
        for k in range(EARLY):
            send(k)

    for c, s in enumerate(chosen[-1]):
        here = pl.ds(s, 1)
        amount = area[here, :] * frac[here, :] * mask[here, :].astype(jnp.float32)
        received[c] = flux[s] * amount

    source_units = jnp.zeros((fields, width), jnp.int32)
    for s in range(blocks):
        here = pl.ds(s, 1)
        amount = area[here, :] * frac[here, :] * mask[here, :].astype(jnp.float32)
        units = (flux[s] * amount * quantum).astype(jnp.int32)
        for r in range(band):
            source_units += units[:, r * width : (r + 1) * width]

    for load in loads[5:]:
        load.wait()
    wetf[...] = wet[...].astype(jnp.float32)
    inverse[...] = wetf[...] / sea[...]
    area_units = jnp.zeros((8, width), jnp.int32)
    for i in range(rows // 8):
        part = pl.ds(i * 8, 8)
        area_units += (sea[part, :] * wetf[part, :] * quantum).astype(jnp.int32)

    held = [any(e[2] for e in plan) for plan in plans[n_lon:]]
    frees = mine_of(held + [False] * n_lon)
    if n_lat > 1 and any(held):
        @pl.when(frees == 1)
        def _():
            first_part.wait_send()
            pl.semaphore_signal(
                go, inc=1, device_id={"lat": my_lat + 1, "lon": me}, device_id_type=MESH
            )

    @pl.when(kind == 1)
    def _():
        for k in range(EARLY, entries):
            send(k)

    sub = lax.broadcasted_iota(jnp.int32, (8, lanes), 0)
    lane = lax.broadcasted_iota(jnp.int32, (8, lanes), 1)

    def placed(values, first):
        return sum(
            jnp.where(lane == sub + (first + i) * 8, v, 0.0) for i, v in enumerate(values)
        )

    firsts_row = placed(row_limbs(source_units) + row_limbs(area_units), 0)
    tally[pl.ds(0, 1), :] = jnp.sum(firsts_row, axis=0, keepdims=True)
    power = jnp.zeros((8, lanes), jnp.int32)
    power_row = jnp.zeros((1, lanes), jnp.int32)
    for f in range(fields):
        power = jnp.where(sub == f, exps[f], power)
        power_row = jnp.where(lane[:1] == f, exps[f], power_row)
    scaling = jnp.left_shift(jnp.ones_like(power), power).astype(jnp.float32)
    scaling_row = jnp.left_shift(jnp.ones_like(power_row), power_row).astype(jnp.float32)

    low = me * blocks
    slot_of = [jnp.int32(0)] * blocks
    near_first = sorted(range(n_lon), key=lambda d: min(d, n_lon - d))
    found = {}
    for d in near_first:
        if len(found) == 1:
            all_of(routes.at[pl.ds(1, n_lon - 1)], route_send, route_recv).wait_recv()
        found[d] = digits_of(d, low, lambda s, row: row)
        for c in range(cap):
            for n in range(blocks):
                slot_of[n] = jnp.where(found[d][c] == n + 1, d * cap + c, slot_of[n])

    def spread(base, recv):
        for lon in range(n_lon):
            for lat in range(n_lat):
                offset = lax.rem(lat - my_lat + n_lat, n_lat) * n_lon + lax.rem(lon - me + n_lon, n_lon)
                pl.when(offset > 0)(pltpu.make_async_remote_copy(
                    src_ref=tally.at[pl.ds(base, 1)], dst_ref=tally.at[pl.ds(base + offset, 1)],
                    send_sem=tally_send, recv_sem=recv,
                    device_id={"lat": jnp.int32(lat), "lon": jnp.int32(lon)}, device_id_type=MESH,
                ).start)
        return all_of(tally.at[pl.ds(base + 1, group - 1)], tally_send, recv)

    early_rows = spread(0, early_recv)

    target_units = jnp.zeros((fields, width), jnp.int32)
    for d in near_first:
        if d:
            all_of(received.at[pl.ds(d * cap, cap)], bulk_send[0], bulk_recv.at[d - 1]).wait_recv()
        for c in range(cap):
            row = jnp.maximum(found[d][c] - 1, 0)
            for r in range(band):
                cover = wetf[pl.ds(row * band + r, 1), :]
                value = received[d * cap + c, :, r * width : (r + 1) * width]
                units = (cover * value * quantum).astype(jnp.int32)
                if not full:
                    units = units * jnp.minimum(found[d][c], 1)
                target_units += units

    tally[pl.ds(group, 1), :] = jnp.sum(placed(row_limbs(target_units), 0), axis=0, keepdims=True)
    late_rows = spread(group, late_recv)
    for n in range(blocks):
        slot = slot_of[n]
        for r in range(band):
            line = n * band + r
            value = received[slot, :, r * width : (r + 1) * width]
            ordered[pl.ds(line, fields, stride=rows), :] = value * (inverse[line : line + 1, :] * scaling)

    def taken(whole, i):
        return jnp.sum(jnp.where(lane == sub + i * 8, whole, 0.0), axis=1, keepdims=True)

    early_rows.wait_recv()
    whole = jnp.sum(tally[pl.ds(0, group), :], axis=0, keepdims=True)
    source = join(taken(whole, 0), taken(whole, 1))
    wet_upper, wet_lower = carry(taken(whole, 2), taken(whole, 3))
    wet_area = join(
        jnp.sum(wet_upper, axis=0, keepdims=True), jnp.sum(wet_lower, axis=0, keepdims=True)
    )
    share = scaling / wet_area
    total_ref[...] = join(whole, pltpu.roll(whole, lanes - 8, 1)) * scaling_row

    late_rows.wait_recv()
    whole = jnp.sum(tally[pl.ds(group, group), :], axis=0, keepdims=True)
    target = join(taken(whole, 0), taken(whole, 1))
    coefs[...] = jnp.broadcast_to((source - target) * share, (fields, lanes))

    all_of(tally.at[pl.ds(0, 2 * (group - 1))], tally_send, late_recv).wait_send()
    all_of(routes.at[pl.ds(1, n_lon - 1)], route_send, route_recv).wait_send()

    @pl.when(frees == 0)
    def _():
        first_part.wait_send()

    rest_part.wait_send()


def finish(ordered, wetf, coefs, total_row, out_hbm, total_hbm, out, total, sems):
    fields = total.shape[0]
    rows = wetf.shape[0]
    total[...] = total_row[0, :fields]
    row = pltpu.make_async_copy(total, total_hbm, sems.at[0])
    row.start()
    for f in range(fields):
        here = pl.ds(f * rows, rows)
        out[here, :] = ordered[here, :] + wetf[...] * coefs[f : f + 1, :]
        pltpu.make_async_copy(out.at[here], out_hbm.at[here], sems.at[1]).start()
    row.wait()
    pltpu.make_async_copy(out, out_hbm, sems.at[1]).wait()


def solution(mesh):
    n_lat, n_lon = mesh.shape["lat"], mesh.shape["lon"]

    def body(ice_flux, ice_frac, ice_mask, ice_area, route, ocean_area, ocean_wet, exponent):
        blocks, fields, cells = ice_flux.shape[1:]
        rows, width = ocean_area.shape
        cap = max(2, blocks // n_lon)
        group = n_lat * n_lon
        anywhere = pl.BlockSpec(memory_space=pl.ANY)
        vmem = pl.BlockSpec(memory_space=pltpu.VMEM)
        dma = pltpu.SemaphoreType.DMA
        near = pl.pallas_call(
            functools.partial(kernel, n_lat, n_lon, cap),
            out_shape=(
                pltpu.VMEM((fields * rows, width), jnp.float32),
                pltpu.VMEM((rows, width), jnp.float32),
                pltpu.VMEM((fields, lanes), jnp.float32),
                pltpu.VMEM((1, lanes), jnp.float32),
            ),
            in_specs=[anywhere] * 8,
            out_specs=(vmem,) * 4,
            scratch_shapes=[
                pltpu.VMEM((blocks, fields, cells), jnp.float32),
                pltpu.VMEM((blocks, cells), jnp.float32),
                pltpu.VMEM((blocks, cells), jnp.int32),
                pltpu.VMEM((blocks, cells), jnp.float32),
                pltpu.VMEM((rows, width), jnp.float32),
                pltpu.VMEM((rows, width), jnp.int32),
                pltpu.VMEM((rows, width), jnp.float32),
                pltpu.VMEM((n_lon * cap, fields, cells), jnp.float32),
                pltpu.VMEM((n_lon * cap, fields, cells), jnp.float32),
                pltpu.SMEM((n_lon, blocks), jnp.int32),
                pltpu.SMEM((fields,), jnp.int32),
                pltpu.VMEM((2 * group, lanes), jnp.float32),
                dma((8,)),
                dma, dma((n_lon - 1,)), dma, dma,
                pltpu.SemaphoreType.REGULAR, pltpu.SemaphoreType.REGULAR,
            ],
            compiler_params=pltpu.CompilerParams(collective_id=0, has_side_effects=True),
        )(
            ice_flux[0], ice_frac[0], ice_mask[0], ice_area[0],
            route, ocean_area, ocean_wet, exponent,
        )
        flux_out, total = pl.pallas_call(
            finish,
            out_shape=(
                jax.ShapeDtypeStruct((fields * rows, width), jnp.float32),
                jax.ShapeDtypeStruct((fields,), jnp.float32),
            ),
            in_specs=[vmem] * 4,
            out_specs=(anywhere, anywhere),
            scratch_shapes=[
                pltpu.VMEM((fields * rows, width), jnp.float32),
                pltpu.VMEM((fields,), jnp.float32),
                dma((2,)),
            ],
        )(*(pltpu.with_memory_space_constraint(x, pltpu.VMEM) for x in near))
        return flux_out.reshape(fields, rows, width), total

    placed = (
        P(("member", "lat"), "lon", None, None),
        P(("member", "lat"), "lon", None),
        P(("member", "lat"), "lon", None),
        P(("member", "lat"), "lon", None),
        P(("member", "lat"), "lon"),
        P(("member", "lat"), "lon"),
        P(("member", "lat"), "lon"),
        P(),
    )
    return jax.shard_map(
        body,
        mesh=mesh,
        in_specs=placed,
        out_specs=(P(None, ("member", "lat"), "lon"), P("member")),
        check_vma=False,
    )
```

```python
import functools

import jax
import jax.numpy as jnp
from jax import lax
from jax.experimental import pallas as pl
from jax.experimental.pallas import tpu as pltpu
from jax.sharding import PartitionSpec as P

MESH = pl.DeviceIdType.MESH
quantum = 1024.0
limb_bits = 16
limb_base = 65536.0
lanes = 128


def carry(upper, lower):
    over = jnp.floor(lower * (1.0 / limb_base))
    return upper + over, lower - over * limb_base


def row_limbs(units):
    upper = jnp.sum((units >> limb_bits).astype(jnp.float32), axis=1, keepdims=True)
    lower = jnp.sum((units & 0xFFFF).astype(jnp.float32), axis=1, keepdims=True)
    return carry(upper, lower)


def join(upper, lower):
    return (upper * limb_base + lower) / quantum


PLANS = {
    4: (
        (4, 6, 7, 5, 2, 3),
        (4, 6, 7, 0, 1, 5),
        (2, 3, 0, 1, 6, 7),
        (2, 3, 0, 1, 4, 5),
        (2, 4, 6, -8, 5, 3),
        (0, 4, 5, 6, -8, 1),
        (2, 0, 1, 3, 6, 7),
        (2, 0, 1, 3, 4, 5),
    ),
}
EARLY = 3
PARTS = 2


def send_plan(count):
    rows = PLANS.get(count)
    if rows is None:
        rows = [
            [
                target * PARTS + half
                for target in sorted((p for p in range(count) if p != me), key=lambda p: -abs(p - me))
                for half in range(PARTS)
            ]
            for _ in range(2)
            for me in range(count)
        ]
    codes = [[(code if code >= 0 else ~code, code < 0) for code in row] for row in rows]
    return [[(code // PARTS, code % PARTS, hold) for code, hold in row] for row in codes]


def kernel(
    n_lat, n_lon, cap,
    flux_hbm, frac_hbm, mask_hbm, area_hbm, route_hbm, sea_hbm, wet_hbm, exp_hbm,
    ordered, wetf, coefs, total_ref,
    flux, frac, mask, area, sea, wet, inverse, outgoing, received, routes, exps, tally,
    in_sem, route_recv, bulk_recv, early_recv, late_recv, top_in, go,
):
    blocks, fields, cells = flux.shape
    rows, width = sea.shape
    band = cells // width
    bits = blocks.bit_length()
    route_send, tally_send, bulk_send = in_sem.at[1], in_sem.at[2], [in_sem.at[3], in_sem.at[4]]
    digit = (1 << bits) - 1
    full = cap * n_lon == blocks
    group = n_lat * n_lon
    piece = cap // PARTS
    my_lat = lax.axis_index("lat")
    me = lax.axis_index("lon")

    def peer(offset):
        return {
            "lat": lax.rem(my_lat + offset // n_lon, n_lat),
            "lon": lax.rem(me + offset % n_lon, n_lon),
        }

    loads = [
        pltpu.make_async_copy(src, dst, in_sem.at[i])
        for i, (src, dst) in enumerate((
            (route_hbm, routes.at[pl.ds(0, 1)]), (area_hbm, area), (frac_hbm, frac),
            (mask_hbm, mask), (flux_hbm, flux), (sea_hbm, sea), (wet_hbm, wet), (exp_hbm, exps),
        ))
    ]
    for load in loads:
        load.start()

    top = n_lon - 1
    barrier = pltpu.get_barrier_semaphore()
    for offset in range(1, n_lat):
        pl.semaphore_signal(barrier, inc=1, device_id=peer(offset * n_lon), device_id_type=MESH)

    @pl.when(me < top)
    def _():
        for offset in range(1, n_lon):
            pl.semaphore_signal(barrier, inc=1, device_id=peer(offset), device_id_type=MESH)

    @pl.when(me == top)
    def _():
        pl.semaphore_wait(barrier, n_lat + n_lon - 2)
        for z in range(top):
            pl.semaphore_signal(
                top_in, inc=1, device_id={"lat": my_lat, "lon": z}, device_id_type=MESH
            )

    loads[0].wait()

    def digits_of(slot, low, value):
        packed = jnp.int32(0)
        for s in range(blocks):
            r = routes[slot, s]
            hit = (r >= low) & (r < low + blocks)
            packed = jnp.where(hit, (packed << bits) + (value(s, r - low) + 1), packed)
        return [(packed >> (bits * (cap - 1 - c))) & digit for c in range(cap)]

    kind = lax.rem(my_lat, 2) if n_lat > 1 else jnp.int32(0)
    place = kind * n_lon + me

    def mine_of(values):
        out = jnp.int32(values[0])
        for z, v in enumerate(values):
            if v != values[0]:
                out = jnp.where(place == z, jnp.int32(v), out)
        return out

    plans = send_plan(n_lon)
    entries = len(plans[0])
    targets = [mine_of([plan[k][0] for plan in plans]) for k in range(entries)]
    halves = [mine_of([plan[k][1] for plan in plans]) for k in range(entries)]
    holds = [[plan[k][2] for plan in plans] for k in range(entries)]
    firsts = [
        [plan[k][0] not in [e[0] for e in plan[:k]] for plan in plans] for k in range(entries)
    ]
    order = [list(dict.fromkeys(e[0] for e in plan)) for plan in plans]
    steps = [mine_of([row[i] for row in order]) for i in range(n_lon - 1)]

    def lon_copy(src, dst, send, recv, d, target):
        return pltpu.make_async_remote_copy(
            src_ref=src, dst_ref=dst, send_sem=send, recv_sem=recv,
            device_id={"lat": my_lat, "lon": target}, device_id_type=MESH,
        )

    def route_copy(target):
        d = lax.rem(target - me + n_lon, n_lon)
        return lon_copy(routes.at[pl.ds(0, 1)], routes.at[pl.ds(d, 1)], route_send, route_recv, d, target)

    def bulk_copy(k):
        d = lax.rem(targets[k] - me + n_lon, n_lon)
        return pltpu.make_async_remote_copy(
            src_ref=outgoing.at[pl.ds(targets[k] * cap + halves[k] * piece, piece)],
            dst_ref=received.at[pl.ds(d * cap + halves[k] * piece, piece)],
            send_sem=bulk_send[int(k >= EARLY)], recv_sem=bulk_recv.at[d - 1],
            device_id={"lat": my_lat, "lon": targets[k]}, device_id_type=MESH,
        )

    def all_of(ref, send, recv):
        return pltpu.make_async_remote_copy(
            src_ref=ref, dst_ref=ref, send_sem=send, recv_sem=recv,
            device_id=peer(1), device_id_type=MESH,
        )

    chosen = [
        [jnp.maximum(v - 1, 0) for v in digits_of(0, target * blocks, lambda s, row: s)]
        for target in steps + [me]
    ]
    for load in loads[1:5]:
        load.wait()

    def fill(target, picks):
        for c, s in enumerate(picks):
            here = pl.ds(s, 1)
            amount = area[here, :] * frac[here, :] * mask[here, :].astype(jnp.float32)
            outgoing[target * cap + c] = flux[s] * amount

    bulk = [bulk_copy(k) for k in range(entries)]
    first_part = all_of(outgoing.at[pl.ds(0, EARLY * piece)], bulk_send[0], bulk_recv.at[0])
    rest_part = all_of(
        outgoing.at[pl.ds(0, (entries - EARLY) * piece)], bulk_send[1], bulk_recv.at[0]
    )

    def send(k):
        if any(holds[k]):
            @pl.when(mine_of(holds[k]) == 1)
            def _():
                pl.semaphore_wait(go, 1)

        waits = [
            first and plan[k][0] == top
            for z, (first, plan) in enumerate(zip(firsts[k], plans))
        ]
        if any(waits):
            @pl.when(mine_of(waits) == 1)
            def _():
                pl.semaphore_wait(top_in, 1)

        if all(firsts[k]):
            route_copy(targets[k]).start()
        elif any(firsts[k]):
            @pl.when(mine_of(firsts[k]) == 1)
            def _():
                route_copy(targets[k]).start()

        bulk[k].start()

    fill(steps[0], chosen[0])
    @pl.when(me < top)
    def _():
        pl.semaphore_wait(barrier, n_lat + n_lon - 3)

    @pl.when(kind == 0)
    def _():
        send(0)

    for target, picks in zip(steps[1:], chosen[1:-1]):
        fill(target, picks)

    @pl.when(kind == 0)
    def _():
        for k in range(1, entries):
            send(k)

    @pl.when(kind == 1)
    def _():
        for k in range(EARLY):
            send(k)

    for c, s in enumerate(chosen[-1]):
        here = pl.ds(s, 1)
        amount = area[here, :] * frac[here, :] * mask[here, :].astype(jnp.float32)
        received[c] = flux[s] * amount

    source_units = jnp.zeros((fields, width), jnp.int32)
    for s in range(blocks):
        here = pl.ds(s, 1)
        amount = area[here, :] * frac[here, :] * mask[here, :].astype(jnp.float32)
        units = (flux[s] * amount * quantum).astype(jnp.int32)
        for r in range(band):
            source_units += units[:, r * width : (r + 1) * width]

    for load in loads[5:]:
        load.wait()
    wetf[...] = wet[...].astype(jnp.float32)
    inverse[...] = wetf[...] / sea[...]
    area_units = jnp.zeros((8, width), jnp.int32)
    for i in range(rows // 8):
        part = pl.ds(i * 8, 8)
        area_units += (sea[part, :] * wetf[part, :] * quantum).astype(jnp.int32)

    held = [any(e[2] for e in plan) for plan in plans[n_lon:]]
    frees = mine_of(held + [False] * n_lon)
    if n_lat > 1 and any(held):
        @pl.when(frees == 1)
        def _():
            first_part.wait_send()
            pl.semaphore_signal(
                go, inc=1, device_id={"lat": my_lat + 1, "lon": me}, device_id_type=MESH
            )

    @pl.when(kind == 1)
    def _():
        for k in range(EARLY, entries):
            send(k)

    sub = lax.broadcasted_iota(jnp.int32, (8, lanes), 0)
    lane = lax.broadcasted_iota(jnp.int32, (8, lanes), 1)

    def placed(values, first):
        return sum(
            jnp.where(lane == sub + (first + i) * 8, v, 0.0) for i, v in enumerate(values)
        )

    firsts_row = placed(row_limbs(source_units) + row_limbs(area_units), 0)
    tally[pl.ds(0, 1), :] = jnp.sum(firsts_row, axis=0, keepdims=True)
    power = jnp.zeros((8, lanes), jnp.int32)
    power_row = jnp.zeros((1, lanes), jnp.int32)
    for f in range(fields):
        power = jnp.where(sub == f, exps[f], power)
        power_row = jnp.where(lane[:1] == f, exps[f], power_row)
    scaling = jnp.left_shift(jnp.ones_like(power), power).astype(jnp.float32)
    scaling_row = jnp.left_shift(jnp.ones_like(power_row), power_row).astype(jnp.float32)

    low = me * blocks
    slot_of = [jnp.int32(0)] * blocks
    near_first = sorted(range(n_lon), key=lambda d: min(d, n_lon - d))
    found = {}
    for d in near_first:
        if len(found) == 1:
            all_of(routes.at[pl.ds(1, n_lon - 1)], route_send, route_recv).wait_recv()
        found[d] = digits_of(d, low, lambda s, row: row)
        for c in range(cap):
            for n in range(blocks):
                slot_of[n] = jnp.where(found[d][c] == n + 1, d * cap + c, slot_of[n])

    def spread(base, recv):
        for lon in range(n_lon):
            for lat in range(n_lat):
                offset = lax.rem(lat - my_lat + n_lat, n_lat) * n_lon + lax.rem(lon - me + n_lon, n_lon)
                pl.when(offset > 0)(pltpu.make_async_remote_copy(
                    src_ref=tally.at[pl.ds(base, 1)], dst_ref=tally.at[pl.ds(base + offset, 1)],
                    send_sem=tally_send, recv_sem=recv,
                    device_id={"lat": jnp.int32(lat), "lon": jnp.int32(lon)}, device_id_type=MESH,
                ).start)
        return all_of(tally.at[pl.ds(base + 1, group - 1)], tally_send, recv)

    early_rows = spread(0, early_recv)

    target_units = jnp.zeros((fields, width), jnp.int32)
    for d in near_first:
        if d:
            all_of(received.at[pl.ds(d * cap, cap)], bulk_send[0], bulk_recv.at[d - 1]).wait_recv()
        for c in range(cap):
            row = jnp.maximum(found[d][c] - 1, 0)
            for r in range(band):
                cover = wetf[pl.ds(row * band + r, 1), :]
                value = received[d * cap + c, :, r * width : (r + 1) * width]
                units = (cover * value * quantum).astype(jnp.int32)
                if not full:
                    units = units * jnp.minimum(found[d][c], 1)
                target_units += units

    tally[pl.ds(group, 1), :] = jnp.sum(placed(row_limbs(target_units), 0), axis=0, keepdims=True)
    late_rows = spread(group, late_recv)
    for n in range(blocks):
        slot = slot_of[n]
        for r in range(band):
            line = n * band + r
            value = received[slot, :, r * width : (r + 1) * width]
            ordered[pl.ds(line, fields, stride=rows), :] = value * (inverse[line : line + 1, :] * scaling)

    def taken(whole, i):
        return jnp.sum(jnp.where(lane == sub + i * 8, whole, 0.0), axis=1, keepdims=True)

    early_rows.wait_recv()
    whole = jnp.sum(tally[pl.ds(0, group), :], axis=0, keepdims=True)
    source = join(taken(whole, 0), taken(whole, 1))
    wet_upper, wet_lower = carry(taken(whole, 2), taken(whole, 3))
    wet_area = join(
        jnp.sum(wet_upper, axis=0, keepdims=True), jnp.sum(wet_lower, axis=0, keepdims=True)
    )
    share = scaling / wet_area
    total_ref[...] = join(whole, pltpu.roll(whole, lanes - 8, 1)) * scaling_row

    late_rows.wait_recv()
    whole = jnp.sum(tally[pl.ds(group, group), :], axis=0, keepdims=True)
    target = join(taken(whole, 0), taken(whole, 1))
    coefs[...] = jnp.broadcast_to((source - target) * share, (fields, lanes))

    all_of(tally.at[pl.ds(0, 2 * (group - 1))], tally_send, late_recv).wait_send()
    all_of(routes.at[pl.ds(1, n_lon - 1)], route_send, route_recv).wait_send()

    @pl.when(frees == 0)
    def _():
        first_part.wait_send()

    rest_part.wait_send()


def finish(ordered, wetf, coefs, total_row, out_hbm, total_hbm, out, total, sems):
    fields = total.shape[0]
    rows = wetf.shape[0]
    total[...] = total_row[0, :fields]
    row = pltpu.make_async_copy(total, total_hbm, sems.at[0])
    row.start()
    for f in range(fields):
        here = pl.ds(f * rows, rows)
        out[here, :] = ordered[here, :] + wetf[...] * coefs[f : f + 1, :]
        pltpu.make_async_copy(out.at[here], out_hbm.at[here], sems.at[1]).start()
    row.wait()
    pltpu.make_async_copy(out, out_hbm, sems.at[1]).wait()


def solution(mesh):
    n_lat, n_lon = mesh.shape["lat"], mesh.shape["lon"]

    def body(ice_flux, ice_frac, ice_mask, ice_area, route, ocean_area, ocean_wet, exponent):
        blocks, fields, cells = ice_flux.shape[1:]
        rows, width = ocean_area.shape
        cap = max(2, blocks // n_lon)
        group = n_lat * n_lon
        anywhere = pl.BlockSpec(memory_space=pl.ANY)
        vmem = pl.BlockSpec(memory_space=pltpu.VMEM)
        dma = pltpu.SemaphoreType.DMA
        near = pl.pallas_call(
            functools.partial(kernel, n_lat, n_lon, cap),
            out_shape=(
                pltpu.VMEM((fields * rows, width), jnp.float32),
                pltpu.VMEM((rows, width), jnp.float32),
                pltpu.VMEM((fields, lanes), jnp.float32),
                pltpu.VMEM((1, lanes), jnp.float32),
            ),
            in_specs=[anywhere] * 8,
            out_specs=(vmem,) * 4,
            scratch_shapes=[
                pltpu.VMEM((blocks, fields, cells), jnp.float32),
                pltpu.VMEM((blocks, cells), jnp.float32),
                pltpu.VMEM((blocks, cells), jnp.int32),
                pltpu.VMEM((blocks, cells), jnp.float32),
                pltpu.VMEM((rows, width), jnp.float32),
                pltpu.VMEM((rows, width), jnp.int32),
                pltpu.VMEM((rows, width), jnp.float32),
                pltpu.VMEM((n_lon * cap, fields, cells), jnp.float32),
                pltpu.VMEM((n_lon * cap, fields, cells), jnp.float32),
                pltpu.SMEM((n_lon, blocks), jnp.int32),
                pltpu.SMEM((fields,), jnp.int32),
                pltpu.VMEM((2 * group, lanes), jnp.float32),
                dma((8,)),
                dma, dma((n_lon - 1,)), dma, dma,
                pltpu.SemaphoreType.REGULAR, pltpu.SemaphoreType.REGULAR,
            ],
            compiler_params=pltpu.CompilerParams(collective_id=0, has_side_effects=True),
        )(
            ice_flux[0], ice_frac[0], ice_mask[0], ice_area[0],
            route, ocean_area, ocean_wet, exponent,
        )
        flux_out, total = pl.pallas_call(
            finish,
            out_shape=(
                jax.ShapeDtypeStruct((fields * rows, width), jnp.float32),
                jax.ShapeDtypeStruct((fields,), jnp.float32),
            ),
            in_specs=[vmem] * 4,
            out_specs=(anywhere, anywhere),
            scratch_shapes=[
                pltpu.VMEM((fields * rows, width), jnp.float32),
                pltpu.VMEM((fields,), jnp.float32),
                dma((2,)),
            ],
        )(*(pltpu.with_memory_space_constraint(x, pltpu.VMEM) for x in near))
        return flux_out.reshape(fields, rows, width), total

    placed = (
        P(("member", "lat"), "lon", None, None),
        P(("member", "lat"), "lon", None),
        P(("member", "lat"), "lon", None),
        P(("member", "lat"), "lon", None),
        P(("member", "lat"), "lon"),
        P(("member", "lat"), "lon"),
        P(("member", "lat"), "lon"),
        P(),
    )
    return jax.shard_map(
        body,
        mesh=mesh,
        in_specs=placed,
        out_specs=(P(None, ("member", "lat"), "lon"), P("member")),
        check_vma=False,
    )
```
